32 devices in a mesh: ocn: 4 (over z), lon: 8 (over y, x, core).
Axes of the slice: x: 2, y: 2, z: 4, core: 2. Of those that a mesh axis runs over, the one named last changes fastest.
Arguments:
- ocean_state: bfloat16 [4, 3072, 128], P(None, ('ocn', 'lon')), may hold values from -6 to 6
- ice_cover: bfloat16 [3072, 128], P(('ocn', 'lon')), may hold values from 0 to 1
- ice_temp: bfloat16 [3072, 128], P(('ocn', 'lon')), may hold values from -6 to 6
- sea_mask: int32 [3072, 128], P(('ocn', 'lon')), may hold values from 0 to 1
- remap_tiles: bfloat16 [32, 160, 128, 128], P(('ocn', 'lon')), may hold values from 0 to 0.015625
- source_tile: int32 [32, 32, 5], P(('ocn', 'lon')), may hold values from 0 to 95
- send_block: int32 [32, 32, 5], P(('ocn', 'lon')), may hold values from -1 to 49, as said below
- recv_block: int32 [32, 32, 5], P(('ocn', 'lon')), may hold values from -1 to 49, as said below
- atm_state: float32 [4, 1600, 128], P(None, ('ocn', 'lon')), may hold values from -6 to 6
Outputs:
- ocean_fluxes: float32 [6, 3072, 128], P(None, ('ocn', 'lon'))
- atm_fluxes: float32 [6, 1600, 128], P(None, ('ocn', 'lon'))
The draws below stay inside these ranges and needn't reach their ends.
Inputs may be any that keep to these rules, and one draw needn't show every extreme that they name: `send_block`: -1 marks an empty slot; every slot from a device to itself is filled. recv_block[e, s, c] equals send_block[s, e, c].
All inputs are finite; a program needn't handle non-finite values.
Results may differ from the reference program's by a relative error of at most 0.0019.
Values may be sent and summed in bfloat16 or wider, within the bound.
A program may use at most 64 MiB of HBM per device.

```python
import math
import jax
import jax.numpy as jnp
from jax import lax

TILE = 128
OB_DEV = 96
AB_DEV = 50
CAP = 5
OBT = 3072
ATB = 1600
SLOTS = 160
N_OCN = 4
N_LON = 8
DEVICES = 32


def intersection_table(key):
    base = jax.random.fold_in(key, 31)
    first, second = jax.random.split(base)
    sender = jnp.arange(DEVICES, dtype=jnp.int32)[:, None, None]
    target = jnp.arange(DEVICES, dtype=jnp.int32)[None, :, None]
    rolled = jax.random.randint(first, (DEVICES, DEVICES, CAP), 0, 100)
    limit = jnp.where(target // N_LON == N_OCN - 1, 95, 35)
    filled = (rolled < limit) | (sender == target)
    blocks = jax.random.randint(second, (DEVICES, DEVICES, CAP), 0, AB_DEV)
    return jnp.where(filled, blocks, -1).astype(jnp.int32)


def source_table(key):
    base = jax.random.fold_in(key, 47)
    return jax.random.randint(base, (DEVICES, DEVICES, CAP), 0, OB_DEV).astype(jnp.int32)


def draw_send_block(key, part):
    return intersection_table(key)


def draw_recv_block(key, part):
    return intersection_table(key).transpose(1, 0, 2)


def draw_source_tile(key, part):
    return source_table(key)


def draw_sea_mask(key, part):
    base = jax.random.fold_in(key, 61)
    first, second, third = jax.random.split(base, 3)
    coastal = jax.random.randint(first, (OBT, 1), 0, 100) < 4
    sparse = jax.random.randint(second, (OBT, 1), 0, 11)
    limit = jnp.where(coastal, sparse, 3 * TILE // 4)
    cells = jax.random.randint(third, (OBT, TILE), 0, TILE)
    return (cells < limit).astype(jnp.int32)


def draw_remap_tiles(key, part):
    base = jax.random.fold_in(key, 67)
    first, second, third, fourth = jax.random.split(base, 4)
    sources = source_table(key)
    blocks = intersection_table(key)
    ocean_weak = jax.random.randint(first, (DEVICES, OB_DEV), 0, 100) < 5
    atm_weak = jax.random.randint(second, (DEVICES, AB_DEV), 0, 100) < 5
    sender = jnp.arange(DEVICES, dtype=jnp.int32)[:, None, None]
    target = jnp.arange(DEVICES, dtype=jnp.int32)[None, :, None]
    partial_slot = ocean_weak[sender, sources] | atm_weak[target, jnp.maximum(blocks, 0)] & (blocks >= 0)
    factor = jnp.exp(jax.random.uniform(third, (DEVICES, DEVICES, CAP), jnp.float32, math.log(0.004), math.log(0.04)))
    scale = jnp.where(partial_slot, factor, 1.0).reshape(DEVICES, SLOTS, 1, 1)
    values = jax.random.uniform(fourth, (DEVICES, SLOTS, TILE, TILE), jnp.float32, 0.0, 2.0 / TILE)
    return (values * scale).astype(jnp.bfloat16)


def steps_of(stream_key, shape, cuts, least, top_value):
    level = 1.0
    for dim, blocks in cuts:
        steps = jax.random.uniform(jax.random.fold_in(jax.random.fold_in(stream_key, 6), dim), (blocks,), jnp.float32, least / len(cuts), top_value / len(cuts))
        level = level * jnp.repeat(jnp.exp(steps), shape[dim] // blocks).reshape((-1,) + (1,) * (len(shape) - 1 - dim))
    return level


def bell_draw(key, extent, spread, most, cuts=(), kind=jnp.bfloat16):
    gain = steps_of(key, extent, cuts, -0.22, 0.18) if cuts else 1.0
    result = jax.random.normal(key, extent, jnp.float32) * spread * gain
    return jnp.minimum(jnp.maximum(result, -most), most).astype(kind)


def setup_inputs(seed: int = 0) -> dict:
    key_of = jax.random.split(jax.random.key(seed), 10)
    ocean_state = bell_draw(key_of[0], (4, OBT, TILE), 1.0, 6.0, ((1, 32),))
    ice_cover = jnp.clip(1.0 * jax.random.uniform(key_of[1], (OBT, TILE), jnp.float32) ** steps_of(key_of[1], (OBT, TILE), ((0, 32),), -0.2, 0.2), 0.0, 1.0).astype(jnp.bfloat16)
    ice_temp = bell_draw(key_of[2], (OBT, TILE), 1.0, 6.0, ((0, 32),))
    sea_mask = draw_sea_mask(jax.random.fold_in(key_of[9], 71), 0)
    remap_tiles = draw_remap_tiles(jax.random.fold_in(key_of[9], 71), 0)
    source_tile = draw_source_tile(jax.random.fold_in(key_of[9], 71), 0)
    send_block = draw_send_block(jax.random.fold_in(key_of[9], 71), 0)
    recv_block = draw_recv_block(jax.random.fold_in(key_of[9], 71), 0)
    atm_state = bell_draw(key_of[8], (4, ATB, TILE), 1.0, 6.0, ((1, 32),), jnp.float32)
    return {"ocean_state": ocean_state, "ice_cover": ice_cover, "ice_temp": ice_temp, "sea_mask": sea_mask, "remap_tiles": remap_tiles, "source_tile": source_tile, "send_block": send_block, "recv_block": recv_block, "atm_state": atm_state}


highest = lax.Precision.HIGHEST

def stack_fields(ocean_state, ice_cover, ice_temp, sea_mask):
    sea_frac = sea_mask.astype(jnp.bfloat16)
    fields = jnp.concatenate([ocean_state, ice_cover[None], ice_temp[None]], 0)
    return jnp.concatenate([fields * sea_frac[None], sea_frac[None]], 0)

def bulk_fluxes(gathered, atm_state):
    inverse = 1.0 / jnp.maximum(gathered[6], 0.1)
    surface_temp = gathered[0] * inverse
    current_u = gathered[1] * inverse
    current_v = gathered[2] * inverse
    salinity = gathered[3] * inverse
    ice_frac = gathered[4] * inverse
    ice_surface = gathered[5] * inverse
    slip_east = atm_state[0] - current_u
    slip_north = atm_state[1] - current_v
    wind_speed = jnp.sqrt(slip_east * slip_east + slip_north * slip_north + 0.25)
    open_water = 1.0 - ice_frac
    saturation = 0.5 * jnp.exp(0.2 * surface_temp) * (1.0 - 0.05 * salinity)
    evaporation = 0.3 * open_water * wind_speed * (saturation - atm_state[3])
    heat = 0.3 * wind_speed * (open_water * (surface_temp - atm_state[2]) + ice_frac * (ice_surface - atm_state[2])) + 2.5 * evaporation
    return jnp.stack([0.5 * open_water * wind_speed * slip_east, 0.5 * open_water * wind_speed * slip_north, 0.8 * ice_frac * wind_speed * slip_east, 0.8 * ice_frac * wind_speed * slip_north, heat, evaporation], 0)

def reference(ocean_state, ice_cover, ice_temp, sea_mask, remap_tiles, source_tile, send_block, recv_block, atm_state):
    devices = remap_tiles.shape[0]
    slots = remap_tiles.shape[1]
    stacked = stack_fields(ocean_state, ice_cover, ice_temp, sea_mask)
    per_device = stacked.reshape(7, devices, OB_DEV, TILE).transpose(1, 0, 2, 3)
    sources = source_tile.reshape(devices, slots)
    targets = send_block.reshape(devices, slots)

    def forward(item):
        fields, tiles, sources_one, targets_one = item
        picked = jnp.take(fields, sources_one, axis=1).astype(jnp.float32)
        contrib = jnp.einsum('fsi,sij->sfj', picked, tiles.astype(jnp.float32), precision=highest)
        filled = (targets_one >= 0).astype(jnp.float32)
        return (contrib * filled[:, None, None]).astype(jnp.bfloat16)
    contribs = lax.map(forward, (per_device, remap_tiles, sources, targets))
    arriving = contribs.reshape(devices, devices, CAP, 7, TILE).transpose(1, 0, 2, 3, 4).reshape(devices, slots, 7, TILE)
    atm_dev = atm_state.reshape(4, devices, AB_DEV, TILE).transpose(1, 0, 2, 3)
    incoming = recv_block.reshape(devices, slots)

    def atmosphere(item):
        received, blocks, state = item
        onehot = (blocks[None, :] == jnp.arange(AB_DEV, dtype=jnp.int32)[:, None]).astype(jnp.float32)
        gathered = jnp.einsum('bs,sfj->fbj', onehot, received.astype(jnp.float32), precision=highest)
        fluxes = bulk_fluxes(gathered, state)
        back = jnp.einsum('bs,fbj->sfj', onehot, fluxes, precision=highest).astype(jnp.bfloat16)
        return (fluxes, back)
    fluxes, backs = lax.map(atmosphere, (arriving, incoming, atm_dev))
    returning = backs.reshape(devices, devices, CAP, 6, TILE).transpose(1, 0, 2, 3, 4).reshape(devices, slots, 6, TILE)
    sea_dev = sea_mask.reshape(devices, OB_DEV, TILE)

    def ocean(item):
        received, tiles, sources_one, targets_one, sea_one = item
        filled = (targets_one >= 0).astype(jnp.float32)
        onehot = (sources_one[None, :] == jnp.arange(OB_DEV, dtype=jnp.int32)[:, None]).astype(jnp.float32) * filled[None, :]
        tiles_wide = tiles.astype(jnp.float32)
        terms = jnp.einsum('sfj,sij->sfi', received.astype(jnp.float32), tiles_wide, precision=highest)
        coverage = lax.optimization_barrier(jnp.sum(tiles_wide, axis=2))
        summed = jnp.einsum('bs,sfi->fbi', onehot, terms, precision=highest)
        cover = jnp.dot(onehot, coverage, precision=highest)
        return summed / jnp.maximum(cover, 0.1)[None] * sea_one.astype(jnp.float32)[None]
    ocean_dev = lax.map(ocean, (returning, remap_tiles, sources, targets, sea_dev))
    ocean_fluxes = ocean_dev.transpose(1, 0, 2, 3).reshape(6, devices * OB_DEV, TILE)
    atm_fluxes = fluxes.transpose(1, 0, 2, 3).reshape(6, devices * AB_DEV, TILE)
    return (ocean_fluxes, atm_fluxes)
```

```python
import functools

import jax
import jax.numpy as jnp
from jax import lax
from jax.experimental import pallas as pl
from jax.experimental.pallas import tpu as pltpu
from jax.sharding import PartitionSpec as P

MESH = pl.DeviceIdType.MESH
F32 = jnp.float32
BF16 = jnp.bfloat16
ROWS = 8


def round_up(value, step):
    return (value + step - 1) // step * step


def fluxes_of(gathered, wind_u, wind_v, air_temp, humidity):
    inverse = 1.0 / jnp.maximum(gathered[6], 0.1)
    surface_temp, current_u, current_v, salinity, ice_frac, ice_surface = (
        gathered[f] * inverse for f in range(6)
    )
    slip_east = wind_u - current_u
    slip_north = wind_v - current_v
    speed = jnp.sqrt(slip_east * slip_east + slip_north * slip_north + 0.25)
    open_water = 1.0 - ice_frac
    saturation = 0.5 * jnp.exp(0.2 * surface_temp) * (1.0 - 0.05 * salinity)
    evaporation = 0.3 * open_water * speed * (saturation - humidity)
    heat = (
        0.3
        * speed
        * (open_water * (surface_temp - air_temp) + ice_frac * (ice_surface - air_temp))
        + 2.5 * evaporation
    )
    return (
        0.5 * open_water * speed * slip_east,
        0.5 * open_water * speed * slip_north,
        0.8 * ice_frac * speed * slip_east,
        0.8 * ice_frac * speed * slip_north,
        heat,
        evaporation,
    )


def kernel(
    n_lon, n, cap, ocean_tiles, atm_tiles, unroll,
    state_hbm, cover_hbm, temp_hbm, mask_hbm, tiles_hbm, source_hbm, recv_hbm, atm_hbm,
    ocean_out, atm_out,
    state, ice_cover, ice_temp, mask, tiles, source_v, recv_v, atm,
    picked, arrived, send_one, recv_one, send_two, recv_two,
    in_sems, tile_sems, sent_one, got_one, sent_two, got_two,
):
    atm_rows = round_up(atm_tiles, 8)
    block = cap * ROWS
    groups = n // unroll
    me = lax.axis_index("ocn") * n_lon + lax.axis_index("lon")

    def place(device):
        return (device // n_lon, device % n_lon)

    def peer_of(i):
        away = (i + 1) // 2
        return (me + n // 2 + jnp.where(i % 2 == 0, away, n - away)) % n

    barrier = pltpu.get_barrier_semaphore()

    def greet(i, carry):
        pl.semaphore_signal(
            barrier, inc=1, device_id=place((me + i) % n), device_id_type=MESH
        )
        return carry

    lax.fori_loop(1, n, greet, 0)

    loads = [
        pltpu.make_async_copy(src, dst, in_sems.at[k])
        for k, (src, dst) in enumerate(
            (
                (source_hbm, source_v),
                (mask_hbm, mask),
                (state_hbm, state),
                (cover_hbm, ice_cover),
                (temp_hbm, ice_temp),
                (recv_hbm, recv_v),
                (atm_hbm, atm.at[pl.ds(0, 4 * atm_tiles)]),
            )
        )
    ]
    for load in loads:
        load.start()

    def tile_copy(peer):
        return pltpu.make_async_copy(
            tiles_hbm.at[0, pl.ds(peer * cap, cap)],
            tiles.at[pl.ds(peer * cap, cap)],
            tile_sems.at[peer],
        )

    def fetch(i, carry):
        tile_copy(peer_of(i)).start()
        return carry

    lax.fori_loop(0, n, fetch, 0)

    for c in range(cap):
        picked[pl.ds(c * ROWS + 7, n, stride=block), :] = jnp.zeros(
            (n, picked.shape[1]), F32
        )
    for load in loads[:5]:
        load.wait()
    def pick(target, onehot, fields):
        chosen = onehot.T.astype(BF16)
        for f, field in enumerate(fields):
            rows = jnp.dot(chosen, field.astype(BF16), preferred_element_type=F32)
            for c in range(cap):
                target[pl.ds(c * ROWS + f, n, stride=block), :] = rows[
                    c * n : (c + 1) * n
                ]

    sea = mask[...].astype(F32)
    sources = jnp.concatenate([source_v[c] for c in range(cap)], 1)
    owners = (
        lax.broadcasted_iota(jnp.int32, (ocean_tiles, n * cap), 0) == sources
    ).astype(F32)
    fields = [state[f].astype(F32) * sea for f in range(4)]
    fields += [ice_cover[...].astype(F32) * sea, ice_temp[...].astype(F32) * sea, sea]
    pick(picked, owners, fields)
    owners = owners.astype(BF16)

    def remap(peer):
        tile_copy(peer).wait()
        rows = picked[pl.ds(pl.multiple_of(peer * block, block), block), :]
        parts = []
        for c in range(cap):
            parts.append(
                jnp.dot(
                    rows[c * ROWS : (c + 1) * ROWS].astype(BF16),
                    tiles[peer * cap + c],
                    preferred_element_type=F32,
                )
            )
        send_one[peer] = jnp.concatenate(parts, 0).astype(BF16)

    def copy_to(peer, outbox, inbox, sent, got):
        return pltpu.make_async_remote_copy(
            src_ref=outbox.at[peer],
            dst_ref=inbox.at[me],
            send_sem=sent.at[peer],
            recv_sem=got.at[me],
            device_id=place(peer),
            device_id_type=MESH,
        )

    def copy_from(peer, outbox, inbox, sent, got):
        return pltpu.make_async_remote_copy(
            src_ref=outbox.at[peer],
            dst_ref=inbox.at[peer],
            send_sem=sent.at[peer],
            recv_sem=got.at[peer],
            device_id=place(peer),
            device_id_type=MESH,
        )

    first = (send_one, recv_one, sent_one, got_one)
    second = (send_two, recv_two, sent_two, got_two)

    for u in range(unroll):
        remap(peer_of(u))
    pl.semaphore_wait(barrier, n - 1)

    def forward(g, carry):
        for u in range(unroll):
            remap(peer_of(g * unroll + u))
        for u in range(unroll):
            copy_to(peer_of((g - 1) * unroll + u), *first).start()
        return carry

    lax.fori_loop(1, groups, forward, 0)
    for u in range(unroll - 1):
        copy_to(peer_of((groups - 1) * unroll + u), *first).start()

    for load in loads[5:]:
        load.wait()
    atm[pl.ds(4 * atm_tiles, 4 * (atm_rows - atm_tiles)), :] = jnp.zeros(
        (4 * (atm_rows - atm_tiles), atm.shape[1]), F32
    )
    blocks = jnp.concatenate([recv_v[c] for c in range(cap)], 1)
    onehot = (
        lax.broadcasted_iota(jnp.int32, (atm_rows, n * cap), 0) == blocks
    ).astype(F32)

    def rows_of(f):
        return jnp.concatenate(
            [arrived[pl.ds(c * ROWS + f, n, stride=block), :] for c in range(cap)], 0
        )

    def keep(peer, inbox):
        arrived[pl.ds(pl.multiple_of(peer * block, block), block), :] = inbox[
            peer
        ].astype(F32)

    keep(me, send_one)

    def receive(i, carry):
        peer = (me + i) % n
        copy_from(peer, *first).wait_recv()
        keep(peer, recv_one)
        return carry

    lax.fori_loop(1, n, receive, 0)
    gathered = [
        jnp.dot(onehot.astype(BF16), rows_of(f).astype(BF16), preferred_element_type=F32)
        for f in range(7)
    ]
    air = [atm[pl.ds(k, atm_rows, stride=4), :] for k in range(4)]
    fluxes = fluxes_of(gathered, *air)
    for f, flux in enumerate(fluxes):
        atm_out[f] = flux[:atm_tiles]
    pick(picked, onehot, fluxes + (jnp.ones_like(fluxes[0]),))

    def answer(peer):
        send_two[peer] = picked[
            pl.ds(pl.multiple_of(peer * block, block), block), :
        ].astype(BF16)

    for u in range(unroll):
        answer(peer_of(u))

    def backward(g, carry):
        for u in range(unroll):
            answer(peer_of(g * unroll + u))
        for u in range(unroll):
            copy_to(peer_of((g - 1) * unroll + u), *second).start()
        return carry

    lax.fori_loop(1, groups, backward, 0)
    for u in range(unroll - 1):
        copy_to(peer_of((groups - 1) * unroll + u), *second).start()

    def spread(peer, inbox):
        back = inbox[peer].astype(F32)
        parts = []
        for c in range(cap):
            parts.append(
                lax.dot_general(
                    back[c * ROWS : (c + 1) * ROWS].astype(BF16),
                    tiles[peer * cap + c],
                    (((1,), (1,)), ((), ())),
                    preferred_element_type=F32,
                )
            )
        arrived[pl.ds(pl.multiple_of(peer * block, block), block), :] = jnp.concatenate(
            parts, 0
        )

    def finish(g, carry):
        peers = [peer_of(n - 1 - g * unroll - u) for u in range(unroll)]
        for peer in peers:
            copy_from(peer, *second).wait_recv()
        for peer in peers:
            spread(peer, recv_two)
        return carry

    spread(me, send_two)
    peers = [peer_of(n - 1 - u) for u in range(1, unroll)]
    for peer in peers:
        copy_from(peer, *second).wait_recv()
    for peer in peers:
        spread(peer, recv_two)
    lax.fori_loop(1, groups, finish, 0)

    def total_of(f):
        rows = rows_of(f)
        high = rows.astype(BF16)
        low = (rows - high.astype(F32)).astype(BF16)
        return jnp.dot(owners, high, preferred_element_type=F32) + jnp.dot(
            owners, low, preferred_element_type=F32
        )

    scale = mask[...].astype(F32) / jnp.maximum(total_of(6), 0.1)
    for f in range(6):
        ocean_out[f] = total_of(f) * scale

    def drain(i, carry):
        peer = (me + i) % n
        copy_to(peer, *first).wait_send()
        copy_to(peer, *second).wait_send()
        return carry

    lax.fori_loop(1, n, drain, 0)


def shards(
    ocean_state,
    ice_cover,
    ice_temp,
    sea_mask,
    remap_tiles,
    source_tile,
    send_block,
    recv_block,
    atm_state,
):
    n_lon = lax.axis_size("lon")
    n = lax.axis_size("ocn") * n_lon
    slots = remap_tiles.shape[1]
    cap = slots // n
    ocean_tiles, width = sea_mask.shape
    atm_tiles = atm_state.shape[1]
    atm_rows = round_up(atm_tiles, 8)
    unroll = 4 if n % 4 == 0 else 1
    sources = source_tile.transpose(2, 0, 1)
    receives = recv_block.transpose(2, 0, 1)
    air = atm_state.transpose(1, 0, 2).reshape(4 * atm_tiles, width)
    anywhere = pl.BlockSpec(memory_space=pl.ANY)
    inside = pl.BlockSpec(memory_space=pltpu.VMEM)
    mail = pltpu.VMEM((n, cap * ROWS, width), BF16)
    sems = pltpu.SemaphoreType.DMA((n,))
    return pl.pallas_call(
        functools.partial(kernel, n_lon, n, cap, ocean_tiles, atm_tiles, unroll),
        out_shape=(
            jax.ShapeDtypeStruct((6, ocean_tiles, width), F32),
            jax.ShapeDtypeStruct((6, atm_tiles, width), F32),
        ),
        in_specs=[anywhere] * 8,
        out_specs=(inside, inside),
        scratch_shapes=[
            pltpu.VMEM(ocean_state.shape, BF16),
            pltpu.VMEM(ice_cover.shape, BF16),
            pltpu.VMEM(ice_temp.shape, BF16),
            pltpu.VMEM(sea_mask.shape, jnp.int32),
            pltpu.VMEM(remap_tiles.shape[1:], BF16),
            pltpu.VMEM(sources.shape, jnp.int32),
            pltpu.VMEM(receives.shape, jnp.int32),
            pltpu.VMEM((4 * atm_rows, width), F32),
            pltpu.VMEM((slots * ROWS, width), F32),
            pltpu.VMEM((slots * ROWS, width), F32),
            mail, mail, mail, mail,
            pltpu.SemaphoreType.DMA((7,)),
            sems, sems, sems, sems, sems,
        ],
        compiler_params=pltpu.CompilerParams(
            collective_id=0, has_side_effects=True, vmem_limit_bytes=60 * 1024 * 1024
        ),
    )(ocean_state, ice_cover, ice_temp, sea_mask, remap_tiles, sources, receives, air)


def solution(mesh):
    one = P(("ocn", "lon"), None)
    field = P(None, ("ocn", "lon"), None)
    slot = P(("ocn", "lon"), None, None)
    return jax.shard_map(
        shards,
        mesh=mesh,
        in_specs=(
            field, one, one, one,
            P(("ocn", "lon"), None, None, None),
            slot, slot, slot, field,
        ),
        out_specs=(field, field),
        check_vma=False,
    )
```
